16 devices in a mesh: tp: 2 (over z), fsdp: 8 (over y, x, core).
Axes of the slice: x: 2, y: 2, z: 2, core: 2. Of those that a mesh axis runs over, the one named last changes fastest.
Arguments:
- x_act: bfloat16 [128, 256, 3072], P('fsdp', 'tp')
- rms_gain: float32 [3072], replicated
- w_query: bfloat16 [3072, 3072], P('fsdp', 'tp')
- w_key: bfloat16 [3072, 1024], P('fsdp', 'tp')
- w_value: bfloat16 [3072, 1024], P('fsdp', 'tp')
- w_out: bfloat16 [3072, 3072], P('tp', 'fsdp')
- dy_out: bfloat16 [128, 256, 3072], P('fsdp', 'tp')
Outputs:
- output 1: bfloat16 [128, 256, 3072], P('fsdp', 'tp')
- output 2: bfloat16 [128, 256, 3072], P('fsdp', 'tp')
- output 3: bfloat16 [3072, 3072], P('fsdp', 'tp')
- output 4: bfloat16 [3072, 1024], P('fsdp', 'tp')
- output 5: bfloat16 [3072, 1024], P('fsdp', 'tp')
- output 6: bfloat16 [3072, 3072], P('tp', 'fsdp')
- output 7: float32 [3072], replicated
All inputs are finite; a program needn't handle non-finite values.
Results may differ from the reference program's by a relative error of at most 0.0184875.
Values are sent between devices in bfloat16 or wider.
A program may use at most 1 GiB of HBM per device.

```python
import jax
import jax.numpy as jnp
from jax import lax

BATCH_SIZE = 128
SEQ_LEN = 256
MODEL_DIM = 3072
Q_HEADS = 24
KV_HEADS = 8
HEAD_DIM = 128
NORM_EPS = 1e-5
ROPE_THETA = 5.0e5
INV_FREQ = tuple(ROPE_THETA ** (-2.0 * pair_idx / HEAD_DIM) for pair_idx in range(HEAD_DIM // 2))


def setup_inputs(seed: int = 0) -> dict:
    rng_keys = jax.random.split(jax.random.key(seed), 7)
    q_cols = Q_HEADS * HEAD_DIM
    kv_cols = KV_HEADS * HEAD_DIM
    act_shape = (BATCH_SIZE, SEQ_LEN, MODEL_DIM)
    x_scale = 3.0 * SEQ_LEN ** -0.5
    x_act = (x_scale * jax.random.normal(rng_keys[0], act_shape, jnp.float32)).astype(jnp.bfloat16)
    rms_gain = 1.0 + 0.3 * jax.random.normal(rng_keys[1], (MODEL_DIM,), jnp.float32)
    w_query = (MODEL_DIM ** -0.5 * jax.random.normal(rng_keys[2], (MODEL_DIM, q_cols), jnp.float32)).astype(jnp.bfloat16)
    w_key = (MODEL_DIM ** -0.5 * jax.random.normal(rng_keys[3], (MODEL_DIM, kv_cols), jnp.float32)).astype(jnp.bfloat16)
    w_value = (MODEL_DIM ** -0.5 * jax.random.normal(rng_keys[4], (MODEL_DIM, kv_cols), jnp.float32)).astype(jnp.bfloat16)
    w_out = (q_cols ** -0.5 * jax.random.normal(rng_keys[5], (q_cols, MODEL_DIM), jnp.float32)).astype(jnp.bfloat16)
    dy_out = jax.random.normal(rng_keys[6], act_shape, jnp.float32).astype(jnp.bfloat16)
    return dict(x_act=x_act, rms_gain=rms_gain, w_query=w_query, w_key=w_key, w_value=w_value, w_out=w_out, dy_out=dy_out)


def rope_tables():
    positions = jnp.arange(SEQ_LEN, dtype=jnp.float32)
    angles = positions[:, None] * jnp.asarray(INV_FREQ, dtype=jnp.float32)[None, :]
    return jnp.cos(angles), jnp.sin(angles)


def apply_rope(head_vals, cos_tab, sin_tab):
    half_dim = HEAD_DIM // 2
    vals_f = head_vals.astype(jnp.float32)
    first_half = vals_f[..., :half_dim]
    second_half = vals_f[..., half_dim:]
    cos_b = cos_tab[:, None, :]
    sin_b = sin_tab[:, None, :]
    rotated = jnp.concatenate([first_half * cos_b - second_half * sin_b, second_half * cos_b + first_half * sin_b], axis=-1)
    return rotated.astype(jnp.bfloat16)


def attend_sequence(operands):
    query_seq, key_seq, value_seq = operands
    q_per_kv = Q_HEADS // KV_HEADS
    query_grp = query_seq.reshape(SEQ_LEN, KV_HEADS, q_per_kv, HEAD_DIM)
    scores = jnp.einsum('qcgd,kcd->cgqk', query_grp.astype(jnp.float32), key_seq.astype(jnp.float32)) * HEAD_DIM ** -0.5
    causal = jnp.arange(SEQ_LEN)[:, None] >= jnp.arange(SEQ_LEN)[None, :]
    attn_prob = jax.nn.softmax(jnp.where(causal, scores, -1e30), axis=-1).astype(jnp.bfloat16)
    attn_mixed = jnp.einsum('cgqk,kcd->qcgd', attn_prob.astype(jnp.float32), value_seq.astype(jnp.float32))
    return attn_mixed.astype(jnp.bfloat16).reshape(SEQ_LEN, Q_HEADS * HEAD_DIM)


def block_forward(x_act, rms_gain, w_query, w_key, w_value, w_out):
    tokens = BATCH_SIZE * SEQ_LEN
    x_f = x_act.astype(jnp.float32)
    inv_rms = lax.rsqrt(jnp.mean(x_f * x_f, axis=-1, keepdims=True) + NORM_EPS)
    normed = (x_f * inv_rms * rms_gain).astype(jnp.bfloat16).reshape(tokens, MODEL_DIM)
    q_proj = jnp.dot(normed, w_query, preferred_element_type=jnp.float32).astype(jnp.bfloat16)
    k_proj = jnp.dot(normed, w_key, preferred_element_type=jnp.float32).astype(jnp.bfloat16)
    v_proj = jnp.dot(normed, w_value, preferred_element_type=jnp.float32).astype(jnp.bfloat16)
    cos_tab, sin_tab = rope_tables()
    queries = apply_rope(q_proj.reshape(BATCH_SIZE, SEQ_LEN, Q_HEADS, HEAD_DIM), cos_tab, sin_tab)
    keys_rot = apply_rope(k_proj.reshape(BATCH_SIZE, SEQ_LEN, KV_HEADS, HEAD_DIM), cos_tab, sin_tab)
    values = v_proj.reshape(BATCH_SIZE, SEQ_LEN, KV_HEADS, HEAD_DIM)
    attn_mixed = lax.map(jax.checkpoint(attend_sequence), (queries, keys_rot, values))
    out_proj = jnp.dot(attn_mixed.reshape(tokens, Q_HEADS * HEAD_DIM), w_out, preferred_element_type=jnp.float32).astype(jnp.bfloat16)
    return (x_f + out_proj.reshape(BATCH_SIZE, SEQ_LEN, MODEL_DIM).astype(jnp.float32)).astype(jnp.bfloat16)


def reference(x_act, rms_gain, w_query, w_key, w_value, w_out, dy_out):
    y_out, pullback = jax.vjp(block_forward, x_act, rms_gain, w_query, w_key, w_value, w_out)
    dx_out, d_rms_gain, dw_query, dw_key, dw_value, dw_out = pullback(dy_out)
    return (y_out, dx_out, dw_query, dw_key, dw_value, dw_out, d_rms_gain)
```

```python
import functools

import jax
import jax.numpy as jnp
from jax import lax
from jax.experimental import pallas as pl
from jax.experimental.pallas import tpu as pltpu
from jax.sharding import PartitionSpec as P


HEAD_DIM = 128
NORM_EPS = 1e-5
ROPE_THETA = 5.0e5
INV_FREQ = tuple(ROPE_THETA ** (-2.0 * pair_idx / HEAD_DIM) for pair_idx in range(HEAD_DIM // 2))
SCALE = HEAD_DIM ** -0.5
GROUPS = 2
F32 = jnp.float32
BF16 = jnp.bfloat16

VMEM_LIMIT = 56 * 1024 * 1024


def cost(flops, moved):
    return pl.CostEstimate(flops=flops, bytes_accessed=moved, transcendentals=0)


def dot_nn(a, b):
    return lax.dot_general(a, b, (((1,), (0,)), ((), ())), preferred_element_type=F32)


def dot_nt(a, b):
    return lax.dot_general(a, b, (((1,), (1,)), ((), ())), preferred_element_type=F32)


def dot_tn(a, b):
    return lax.dot_general(a, b, (((0,), (0,)), ((), ())), preferred_element_type=F32)


def rope_tables(seq_len):
    positions = jnp.arange(seq_len, dtype=F32)
    angles = positions[:, None] * jnp.asarray(INV_FREQ, dtype=F32)[None, :]
    cos, sin = jnp.cos(angles), jnp.sin(angles)
    return jnp.concatenate([cos, cos], axis=1), jnp.concatenate([-sin, sin], axis=1)


def swap_halves(vals):
    return pltpu.roll(vals, HEAD_DIM // 2, 1)


def attend_kernel(per_kv, n_kv, n_half, second_ref, tab_ref, *refs):
    q_refs, kv_refs, do_refs, kvx_refs = (refs[i * n_half:(i + 1) * n_half] for i in range(4))
    mixed_ref, dq_ref, dkv_own_ref, dkv_prev_ref = refs[4 * n_half:]
    seq = tab_ref.shape[1]
    kw = n_kv * HEAD_DIM

    def rope(vals, tab):
        vals_f = vals.astype(F32)
        return (vals_f * tab_ref[tab] + swap_halves(vals_f) * tab_ref[tab + 1]).astype(BF16)

    def unrope(vals, tab):
        return vals * tab_ref[tab] - swap_halves(vals) * tab_ref[tab + 1]

    def unit(half, kv, cross):
        cols = slice(kv * HEAD_DIM, (kv + 1) * HEAD_DIM)
        vcols = slice(kw + kv * HEAD_DIM, kw + (kv + 1) * HEAD_DIM)
        heads = [slice((kv * per_kv + i) * HEAD_DIM, (kv * per_kv + i + 1) * HEAD_DIM) for i in range(per_kv)]
        q = jnp.concatenate([rope(q_refs[half][:, h], 0) for h in heads], axis=0)
        d_out = jnp.concatenate([do_refs[half][:, h] for h in heads], axis=0)
        keys = rope(kv_refs[half][:, cols], 0)
        vals = kv_refs[half][:, vcols]
        key_pos = lax.broadcasted_iota(jnp.int32, (seq, seq), 0)
        query_pos = lax.broadcasted_iota(jnp.int32, (seq, seq), 1)
        causal = jnp.concatenate([key_pos <= query_pos] * per_kv, axis=1)
        if cross:
            keys = jnp.concatenate([keys, rope(kvx_refs[half][:, cols], 2)], axis=0)
            vals = jnp.concatenate([vals, kvx_refs[half][:, vcols]], axis=0)
        scores = dot_nt(keys, q) * SCALE
        own = jnp.where(causal, scores[:seq], -1e30)
        scores = jnp.concatenate([own, scores[seq:]], axis=0) if cross else own
        top = jnp.max(scores, axis=0, keepdims=True)
        weights = jnp.exp(scores - top)
        prob = weights * (1.0 / jnp.sum(weights, axis=0, keepdims=True))
        prob_bf = prob.astype(BF16)
        d_prob = dot_nt(vals, d_out)
        d_sum = jnp.sum(prob * d_prob, axis=0, keepdims=True)
        d_scores = ((prob * (d_prob - d_sum)) * SCALE).astype(BF16)
        mixed = dot_tn(prob_bf, vals).astype(BF16)
        d_q = dot_tn(d_scores, keys)
        d_vals = dot_nn(prob_bf, d_out)
        d_keys = dot_nn(d_scores, q)
        for i, h in enumerate(heads):
            rows = slice(i * seq, (i + 1) * seq)
            mixed_ref[half, :, h] = mixed[rows]
            dq_ref[half, :, h] = unrope(d_q[rows], 0).astype(BF16)
        dkv_own_ref[half, :, cols] = unrope(d_keys[:seq], 0)
        dkv_own_ref[half, :, vcols] = d_vals[:seq]
        if cross:
            dkv_prev_ref[half, :, cols] = unrope(d_keys[seq:], 2).astype(BF16)
            dkv_prev_ref[half, :, vcols] = d_vals[seq:].astype(BF16)

    def run(cross):
        for half in range(n_half):
            for kv in range(n_kv):
                unit(half, kv, cross)

    @pl.when(second_ref[0] == 0)
    def _():
        run(False)
        dkv_prev_ref[...] = jnp.zeros_like(dkv_prev_ref)

    @pl.when(second_ref[0] != 0)
    def _():
        run(True)


def attend(seq, second, tables, q, kv, d_mixed, kv_prev):
    n_half = len(q)
    tokens, qw = q[0].shape
    kw = kv[0].shape[1] // 2
    q_spec = pl.BlockSpec((seq, qw), lambda s: (s, 0))
    kv_spec = pl.BlockSpec((seq, 2 * kw), lambda s: (s, 0))

    def both(width):
        return pl.BlockSpec((n_half, seq, width), lambda s: (0, s, 0))

    flops = 6 * 2 * tokens * 2 * seq * n_half * qw
    return pl.pallas_call(
        functools.partial(attend_kernel, qw // kw, kw // HEAD_DIM, n_half),
        grid=(tokens // seq,),
        in_specs=[pl.BlockSpec(memory_space=pltpu.SMEM), pl.BlockSpec(tables.shape, lambda s: (0, 0, 0))]
        + [q_spec] * n_half + [kv_spec] * n_half + [q_spec] * n_half + [kv_spec] * n_half,
        out_specs=[both(qw), both(qw), both(2 * kw), both(2 * kw)],
        out_shape=[jax.ShapeDtypeStruct((n_half, tokens, qw), BF16), jax.ShapeDtypeStruct((n_half, tokens, qw), BF16),
                   jax.ShapeDtypeStruct((n_half, tokens, 2 * kw), F32), jax.ShapeDtypeStruct((n_half, tokens, 2 * kw), BF16)],
        compiler_params=pltpu.CompilerParams(dimension_semantics=("arbitrary",), vmem_limit_bytes=VMEM_LIMIT),
        cost_estimate=cost(4 * flops, n_half * tokens * (8 * qw + 14 * kw)),
        name="attend",
    )(second, tables, *q, *kv, *d_mixed, *kv_prev)


def prepare_kernel(x_ref, dy_ref, gain_ref, h_ref, ht_ref, dyt_ref):
    x_f = x_ref[...].astype(F32)
    inv_rms = lax.rsqrt(jnp.mean(x_f * x_f, axis=-1, keepdims=True) + NORM_EPS)
    h = (x_f * inv_rms * gain_ref[...]).astype(BF16)
    h_ref[...] = h
    ht_ref[...] = h.T
    dyt_ref[...] = dy_ref[...].T


def prepare(x, dy, gain):
    tokens, dim = x.shape
    block = 128
    row_spec = pl.BlockSpec((block, dim), lambda s: (s, 0))
    col_spec = pl.BlockSpec((dim, block), lambda s: (0, s))
    return pl.pallas_call(
        prepare_kernel,
        grid=(tokens // block,),
        in_specs=[row_spec, row_spec, pl.BlockSpec((1, dim), lambda s: (0, 0))],
        out_specs=[row_spec, col_spec, col_spec],
        out_shape=[jax.ShapeDtypeStruct((tokens, dim), BF16)] + [jax.ShapeDtypeStruct((dim, tokens), BF16)] * 2,
        compiler_params=pltpu.CompilerParams(dimension_semantics=("arbitrary",), vmem_limit_bytes=VMEM_LIMIT),
        cost_estimate=cost(60 * tokens * dim, 10 * tokens * dim),
        name="prepare",
    )(x, dy, gain.reshape(1, dim))


def weight_grad_kernel(at_ref, b_ref, out_ref):
    out_ref[0] = dot_nn(at_ref[...], b_ref[0])


def weight_grad(at, b):
    dim, tokens = at.shape
    n_half, _, width = b.shape
    rows = min(1024, dim)
    return pl.pallas_call(
        weight_grad_kernel,
        grid=(n_half, dim // rows),
        in_specs=[pl.BlockSpec((rows, tokens), lambda z, m: (m, 0)), pl.BlockSpec((1, tokens, width), lambda z, m: (z, 0, 0))],
        out_specs=pl.BlockSpec((1, rows, width), lambda z, m: (z, m, 0)),
        out_shape=jax.ShapeDtypeStruct((n_half, dim, width), F32),
        compiler_params=pltpu.CompilerParams(dimension_semantics=("arbitrary", "arbitrary"), vmem_limit_bytes=VMEM_LIMIT),
        cost_estimate=cost(2 * n_half * tokens * dim * width, n_half * (4 * dim * width + 2 * tokens * (width + dim))),
        name="weight_grad",
    )(at, b)


def gather_sum_kernel(n_pairs, n_half, has_res, *refs):
    acts, weights, out_ref = refs[:n_pairs], refs[n_pairs:2 * n_pairs], refs[-1]
    total = None
    for act, weight in zip(acts, weights):
        for half in range(n_half):
            term = dot_nt(act[half], weight[half])
            total = term if total is None else total + term
    rounded = total.astype(BF16)
    if has_res:
        rounded = (refs[2 * n_pairs][...].astype(F32) + rounded.astype(F32)).astype(BF16)
    out_ref[...] = rounded


def project_back(acts, weights, res=None):
    n_half, tokens, _ = acts[0].shape
    dim = weights[0].shape[1]
    bm, bn = min(1024, tokens), 512
    widths = [a.shape[2] for a in acts]
    out_spec = pl.BlockSpec((bm, bn), lambda m, n: (m, n))
    return pl.pallas_call(
        functools.partial(gather_sum_kernel, len(acts), n_half, res is not None),
        grid=(tokens // bm, dim // bn),
        in_specs=[pl.BlockSpec((n_half, bm, w), lambda m, n: (0, m, 0)) for w in widths]
        + [pl.BlockSpec((n_half, bn, w), lambda m, n: (0, n, 0)) for w in widths] + ([] if res is None else [out_spec]),
        out_specs=out_spec,
        out_shape=jax.ShapeDtypeStruct((tokens, dim), BF16),
        compiler_params=pltpu.CompilerParams(dimension_semantics=("arbitrary", "arbitrary"), vmem_limit_bytes=VMEM_LIMIT),
        cost_estimate=cost(2 * tokens * dim * n_half * sum(widths), 2 * n_half * (tokens + 2 * dim) * sum(widths) + 4 * tokens * dim),
        name="project_back",
    )(*acts, *weights, *([] if res is None else [res]))


def input_grad_kernel(x_ref, dy_ref, dh_ref, gain_ref, dx_ref, dgain_ref):
    x_f = x_ref[...].astype(F32)
    d_h = dh_ref[...].astype(F32)
    inv_rms = lax.rsqrt(jnp.mean(x_f * x_f, axis=-1, keepdims=True) + NORM_EPS)
    grad_gain = d_h * gain_ref[...]
    mean_gx = jnp.mean(grad_gain * x_f, axis=-1, keepdims=True)
    dx_ref[...] = (dy_ref[...].astype(F32) + inv_rms * (grad_gain - x_f * inv_rms * inv_rms * mean_gx)).astype(BF16)

    @pl.when(pl.program_id(0) == 0)
    def _():
        dgain_ref[...] = jnp.zeros_like(dgain_ref)

    dgain_ref[...] += jnp.sum(d_h * x_f * inv_rms, axis=0, keepdims=True)


def input_grad(x, dy, d_h, gain):
    tokens, dim = x.shape
    block = 128
    row_spec = pl.BlockSpec((block, dim), lambda s: (s, 0))
    gain_spec = pl.BlockSpec((1, dim), lambda s: (0, 0))
    return pl.pallas_call(
        input_grad_kernel,
        grid=(tokens // block,),
        in_specs=[row_spec, row_spec, row_spec, gain_spec],
        out_specs=[row_spec, gain_spec],
        out_shape=[jax.ShapeDtypeStruct((tokens, dim), BF16), jax.ShapeDtypeStruct((1, dim), F32)],
        compiler_params=pltpu.CompilerParams(dimension_semantics=("arbitrary",), vmem_limit_bytes=VMEM_LIMIT),
        cost_estimate=cost(60 * tokens * dim, 8 * tokens * dim),
        name="input_grad",
    )(x, dy, d_h, gain.reshape(1, dim))


def flip_kernel(w_ref, *out_refs):
    width = w_ref.shape[0] // len(out_refs)
    for i, out_ref in enumerate(out_refs):
        out_ref[...] = w_ref[i * width:(i + 1) * width, :].T


def flip(w, parts):
    rows, cols = w.shape
    shape = jax.ShapeDtypeStruct((cols, rows // parts), BF16)
    return pl.pallas_call(flip_kernel, out_shape=[shape] * parts, cost_estimate=cost(10 * rows * cols, 4 * rows * cols), name="flip")(w)


def finish_kernel(n_parts, splits, *refs):
    parts, outs = refs[:n_parts], refs[n_parts:]
    for p, part in enumerate(parts):
        width = part.shape[1] // splits
        for i, out in enumerate(outs):
            out[:, p * width:(p + 1) * width] = part[:, i * width:(i + 1) * width].astype(BF16)


def finish(parts, splits):
    rows, width = parts[0].shape
    shape = jax.ShapeDtypeStruct((rows, len(parts) * width // splits), BF16)
    return pl.pallas_call(functools.partial(finish_kernel, len(parts), splits), out_shape=[shape] * splits, name="finish",
                          cost_estimate=cost(10 * rows * width, 6 * rows * width))(*parts)


def finish_flip_kernel(*refs):
    parts, out = refs[:-1], refs[-1]
    width = parts[0].shape[1]
    for p, part in enumerate(parts):
        out[p * width:(p + 1) * width, :] = part[...].T.astype(BF16)


def finish_flip(parts):
    rows, width = parts[0].shape
    shape = jax.ShapeDtypeStruct((len(parts) * width, rows), BF16)
    return pl.pallas_call(finish_flip_kernel, out_shape=shape, name="finish_flip",
                          cost_estimate=cost(10 * rows * width, 6 * rows * width))(*parts)


def after(dep, value):
    return lax.optimization_barrier((dep, value))[1]


def solution(mesh):
    tp = mesh.shape['tp']
    everyone = ('tp', 'fsdp')
    act_spec = P('fsdp', 'tp', None)
    col_spec = P('fsdp', 'tp')
    row_spec = P('tp', 'fsdp')

    def shard_body(x_loc, gain, wq_loc, wk_loc, wv_loc, wo_loc, dy_loc):
        batch, seq, dim = x_loc.shape
        tokens = batch * seq
        q_cols, kv_cols = wq_loc.shape[1], wk_loc.shape[1]
        tp_idx = lax.axis_index('tp')

        def gather(block):
            return lax.all_gather(block, everyone, axis=0, tiled=True).reshape(tp, dim, block.shape[1])

        def scatter(parts):
            return lax.psum_scatter(parts.reshape(tp * dim, parts.shape[2]), everyone, scatter_dimension=0, tiled=True)

        kw, qw = kv_cols // GROUPS, q_cols // GROUPS
        wo_flipped = flip(wo_loc, GROUPS)
        wkv, wq, wo = [], [], []
        for g in range(GROUPS):
            ks = slice(g * kw, (g + 1) * kw)
            wkv.append(gather(jnp.concatenate([wk_loc[:, ks], wv_loc[:, ks]], axis=1)))
            wq.append(gather(wq_loc[:, g * qw:(g + 1) * qw]))
            wo.append(gather(wo_flipped[g]))

        x = x_loc.reshape(tokens, dim)
        dy = dy_loc.reshape(tokens, dim)
        normed, normed_t, dy_t = prepare(x, dy, gain)

        cos_tab, sin_tab = rope_tables(seq * tp)
        tables = jnp.stack([lax.dynamic_slice_in_dim(cos_tab, tp_idx * seq, seq), lax.dynamic_slice_in_dim(sin_tab, tp_idx * seq, seq),
                            cos_tab[:seq], sin_tab[:seq]])
        second = tp_idx.astype(jnp.int32).reshape(1)

        def project(act, weights, dep):
            act = after(dep, act)
            return [dot_nn(act, weights[z]).astype(BF16) for z in range(tp)]

        def attend_group(kv_g, kv_prev_g, q_g, d_mixed, dep):
            return attend(seq, second, after(dep, tables), q_g, kv_g, d_mixed, kv_prev_g)

        def send_kv(kv_g):
            return [lax.ppermute(part, 'tp', [(0, 1)]) for part in kv_g]

        def kv_grad(own, prev):
            return (own + lax.ppermute(prev, 'tp', [(1, 0)]).astype(F32)).astype(BF16)

        assert GROUPS == 2
        kv0 = project(normed, wkv[0], normed)
        prev0 = send_kv(kv0)
        q0 = project(normed, wq[0], kv0[-1])
        d_mixed0 = project(dy, wo[0], q0[-1])
        kv1 = project(normed, wkv[1], d_mixed0[-1])
        prev1 = send_kv(kv1)
        mixed0, d_q0, own0, back0 = attend_group(kv0, prev0, q0, d_mixed0, kv1[-1])
        d_kv0 = kv_grad(own0, back0)
        part = weight_grad(after(mixed0, dy_t), mixed0)
        dwo0 = scatter(part)
        part = weight_grad(after(part, normed_t), d_q0)
        dwq0 = scatter(part)
        q1 = project(normed, wq[1], part)
        d_mixed1 = project(dy, wo[1], q1[-1])
        mixed1, d_q1, own1, back1 = attend_group(kv1, prev1, q1, d_mixed1, d_mixed1[-1])
        d_kv1 = kv_grad(own1, back1)
        part = weight_grad(after(mixed1, normed_t), d_kv0)
        dwkv0 = scatter(part)
        part = weight_grad(after(part, dy_t), mixed1)
        dwo1 = scatter(part)
        part = weight_grad(after(part, normed_t), d_q1)
        dwq1 = scatter(part)
        y = project_back([mixed0, mixed1], wo, after(part, x))
        part = weight_grad(after(y, normed_t), d_kv1)
        dwkv1 = scatter(part)
        d_normed = project_back([after(part, d_q0), d_q1, d_kv0, d_kv1], wq + wkv)
        dx, d_gain = input_grad(x, dy, d_normed, gain)
        d_gain = lax.psum(d_gain.reshape(dim), everyone)

        dwo_loc = finish_flip([dwo0, dwo1])
        dwq_loc, = finish([dwq0, dwq1], 1)
        dwk_loc, dwv_loc = finish([dwkv0, dwkv1], 2)
        return (y.reshape(x_loc.shape), dx.reshape(x_loc.shape), dwq_loc, dwk_loc, dwv_loc, dwo_loc, d_gain)

    return jax.shard_map(shard_body, mesh=mesh,
                         in_specs=(act_spec, P(), col_spec, col_spec, col_spec, row_spec, act_spec),
                         out_specs=(act_spec, act_spec, col_spec, col_spec, col_spec, row_spec, P()),
                         check_vma=False)
```

```python
import functools

import jax
import jax.numpy as jnp
from jax import lax
from jax.experimental import pallas as pl
from jax.experimental.pallas import tpu as pltpu
from jax.sharding import Mesh
from jax.sharding import PartitionSpec as P


HEAD_DIM = 128
NORM_EPS = 1e-5
ROPE_THETA = 5.0e5
INV_FREQ = tuple(ROPE_THETA ** (-2.0 * pair_idx / HEAD_DIM) for pair_idx in range(HEAD_DIM // 2))
SCALE = HEAD_DIM ** -0.5
CORES = 2
F32 = jnp.float32
BF16 = jnp.bfloat16

VMEM_LIMIT = 56 * 1024 * 1024


def cost(flops, moved):
    return pl.CostEstimate(flops=flops, bytes_accessed=moved, transcendentals=0)


def dot_nn(a, b):
    return lax.dot_general(a, b, (((1,), (0,)), ((), ())), preferred_element_type=F32)


def dot_nt(a, b):
    return lax.dot_general(a, b, (((1,), (1,)), ((), ())), preferred_element_type=F32)


def dot_tn(a, b):
    return lax.dot_general(a, b, (((0,), (0,)), ((), ())), preferred_element_type=F32)


def rope_tables(seq_len):
    positions = jnp.arange(seq_len, dtype=F32)
    angles = positions[:, None] * jnp.asarray(INV_FREQ, dtype=F32)[None, :]
    cos, sin = jnp.cos(angles), jnp.sin(angles)
    return jnp.concatenate([cos, cos], axis=1), jnp.concatenate([-sin, sin], axis=1)


def swap_halves(vals):
    return pltpu.roll(vals, HEAD_DIM // 2, 1)


def attend_kernel(per_kv, n_kv, n_half, second_ref, tab_ref, *refs):
    q_refs, kv_refs, do_refs, kvx_refs = (refs[i * n_half:(i + 1) * n_half] for i in range(4))
    mixed_ref, dq_ref, dkv_own_ref, dkv_prev_ref = refs[4 * n_half:]
    seq = tab_ref.shape[1]
    kw = n_kv * HEAD_DIM

    def rope(vals, tab):
        vals_f = vals.astype(F32)
        return (vals_f * tab_ref[tab] + swap_halves(vals_f) * tab_ref[tab + 1]).astype(BF16)

    def unrope(vals, tab):
        return vals * tab_ref[tab] - swap_halves(vals) * tab_ref[tab + 1]

    def unit(half, kv, cross):
        cols = slice(kv * HEAD_DIM, (kv + 1) * HEAD_DIM)
        vcols = slice(kw + kv * HEAD_DIM, kw + (kv + 1) * HEAD_DIM)
        heads = [slice((kv * per_kv + i) * HEAD_DIM, (kv * per_kv + i + 1) * HEAD_DIM) for i in range(per_kv)]
        q = jnp.concatenate([rope(q_refs[half][:, h], 0) for h in heads], axis=0)
        d_out = jnp.concatenate([do_refs[half][:, h] for h in heads], axis=0)
        keys = rope(kv_refs[half][:, cols], 0)
        vals = kv_refs[half][:, vcols]
        key_pos = lax.broadcasted_iota(jnp.int32, (seq, seq), 0)
        query_pos = lax.broadcasted_iota(jnp.int32, (seq, seq), 1)
        causal = jnp.concatenate([key_pos <= query_pos] * per_kv, axis=1)
        if cross:
            keys = jnp.concatenate([keys, rope(kvx_refs[half][:, cols], 2)], axis=0)
            vals = jnp.concatenate([vals, kvx_refs[half][:, vcols]], axis=0)
        scores = dot_nt(keys, q) * SCALE
        own = jnp.where(causal, scores[:seq], -1e30)
        scores = jnp.concatenate([own, scores[seq:]], axis=0) if cross else own
        top = jnp.max(scores, axis=0, keepdims=True)
        weights = jnp.exp(scores - top)
        prob = weights * (1.0 / jnp.sum(weights, axis=0, keepdims=True))
        prob_bf = prob.astype(BF16)
        d_prob = dot_nt(vals, d_out)
        d_sum = jnp.sum(prob * d_prob, axis=0, keepdims=True)
        d_scores = ((prob * (d_prob - d_sum)) * SCALE).astype(BF16)
        mixed = dot_tn(prob_bf, vals).astype(BF16)
        d_q = dot_tn(d_scores, keys)
        d_vals = dot_nn(prob_bf, d_out)
        d_keys = dot_nn(d_scores, q)
        for i, h in enumerate(heads):
            rows = slice(i * seq, (i + 1) * seq)
            mixed_ref[half, :, h] = mixed[rows]
            dq_ref[half, :, h] = unrope(d_q[rows], 0).astype(BF16)
        dkv_own_ref[half, :, cols] = unrope(d_keys[:seq], 0)
        dkv_own_ref[half, :, vcols] = d_vals[:seq]
        if cross:
            dkv_prev_ref[half, :, cols] = unrope(d_keys[seq:], 2).astype(BF16)
            dkv_prev_ref[half, :, vcols] = d_vals[seq:].astype(BF16)

    def run(cross):
        for half in range(n_half):
            for kv in range(n_kv):
                unit(half, kv, cross)

    @pl.when(second_ref[0] == 0)
    def _():
        run(False)
        dkv_prev_ref[...] = jnp.zeros_like(dkv_prev_ref)

    @pl.when(second_ref[0] != 0)
    def _():
        run(True)


def attend(seq, second, tables, q, kv, d_mixed, kv_prev):
    n_half = len(q)
    tokens, qw = q[0].shape
    kw = kv[0].shape[1] // 2
    q_spec = pl.BlockSpec((seq, qw), lambda s: (s, 0))
    kv_spec = pl.BlockSpec((seq, 2 * kw), lambda s: (s, 0))

    def both(width):
        return pl.BlockSpec((n_half, seq, width), lambda s: (0, s, 0))

    flops = 6 * 2 * tokens * 2 * seq * n_half * qw
    return pl.pallas_call(
        functools.partial(attend_kernel, qw // kw, kw // HEAD_DIM, n_half),
        grid=(tokens // seq,),
        in_specs=[pl.BlockSpec(memory_space=pltpu.SMEM), pl.BlockSpec(tables.shape, lambda s: (0, 0, 0))]
        + [q_spec] * n_half + [kv_spec] * n_half + [q_spec] * n_half + [kv_spec] * n_half,
        out_specs=[both(qw), both(qw), both(2 * kw), both(2 * kw)],
        out_shape=[jax.ShapeDtypeStruct((n_half, tokens, qw), BF16), jax.ShapeDtypeStruct((n_half, tokens, qw), BF16),
                   jax.ShapeDtypeStruct((n_half, tokens, 2 * kw), F32), jax.ShapeDtypeStruct((n_half, tokens, 2 * kw), BF16)],
        compiler_params=pltpu.CompilerParams(dimension_semantics=("arbitrary",), vmem_limit_bytes=VMEM_LIMIT),
        cost_estimate=cost(4 * flops, n_half * tokens * (8 * qw + 14 * kw)),
        name="attend",
    )(second, tables, *q, *kv, *d_mixed, *kv_prev)


def prepare_kernel(x_ref, dy_ref, gain_ref, h_ref, ht_ref, dyt_ref):
    x_f = x_ref[...].astype(F32)
    inv_rms = lax.rsqrt(jnp.mean(x_f * x_f, axis=-1, keepdims=True) + NORM_EPS)
    h = (x_f * inv_rms * gain_ref[...]).astype(BF16)
    h_ref[...] = h
    ht_ref[...] = h.T
    dyt_ref[...] = dy_ref[...].T


def prepare(x, dy, gain):
    tokens, dim = x.shape
    block = 128
    row_spec = pl.BlockSpec((block, dim), lambda s: (s, 0))
    col_spec = pl.BlockSpec((dim, block), lambda s: (0, s))
    return pl.pallas_call(
        prepare_kernel,
        grid=(tokens // block,),
        in_specs=[row_spec, row_spec, pl.BlockSpec((1, dim), lambda s: (0, 0))],
        out_specs=[row_spec, col_spec, col_spec],
        out_shape=[jax.ShapeDtypeStruct((tokens, dim), BF16)] + [jax.ShapeDtypeStruct((dim, tokens), BF16)] * 2,
        compiler_params=pltpu.CompilerParams(dimension_semantics=("arbitrary",), vmem_limit_bytes=VMEM_LIMIT),
        cost_estimate=cost(60 * tokens * dim, 10 * tokens * dim),
        name="prepare",
    )(x, dy, gain.reshape(1, dim))


def weight_grad_kernel(n_sets, *refs):
    total = None
    for at_ref, b_ref in zip(refs[:n_sets], refs[n_sets:2 * n_sets]):
        term = dot_nn(at_ref[...], b_ref[0])
        total = term if total is None else total + term
    refs[-1][0] = total


def weight_grad(at, b):
    dim, tokens = at[0].shape
    n_half, _, width = b[0].shape
    n_sets = len(at)
    rows = min(1024, dim)
    return pl.pallas_call(
        functools.partial(weight_grad_kernel, n_sets),
        grid=(n_half, dim // rows),
        in_specs=[pl.BlockSpec((rows, tokens), lambda z, m: (m, 0))] * n_sets
        + [pl.BlockSpec((1, tokens, width), lambda z, m: (z, 0, 0))] * n_sets,
        out_specs=pl.BlockSpec((1, rows, width), lambda z, m: (z, m, 0)),
        out_shape=jax.ShapeDtypeStruct((n_half, dim, width), F32),
        compiler_params=pltpu.CompilerParams(dimension_semantics=("arbitrary", "arbitrary"), vmem_limit_bytes=VMEM_LIMIT),
        cost_estimate=cost(2 * n_sets * n_half * tokens * dim * width, n_half * (4 * dim * width + 2 * n_sets * tokens * (width + dim))),
        name="weight_grad",
    )(*at, *b)


def project_back_kernel(n_pairs, n_half, has_part, has_res, *refs):
    acts, weights, rest, out_ref = refs[:n_pairs], refs[n_pairs:2 * n_pairs], list(refs[2 * n_pairs:-1]), refs[-1]
    total = None
    for act, weight in zip(acts, weights):
        for half in range(n_half):
            term = dot_nt(act[half], weight[half])
            total = term if total is None else total + term
    if has_part:
        total = total + rest.pop(0)[...].astype(F32)
    rounded = total.astype(BF16)
    if has_res:
        rounded = (rest.pop(0)[...].astype(F32) + rounded.astype(F32)).astype(BF16)
    out_ref[...] = rounded


def project_back(acts, weights, part=None, res=None):
    n_half, tokens, _ = acts[0].shape
    dim = weights[0].shape[1]
    bm, bn = min(1024, tokens), 512
    widths = [a.shape[2] for a in acts]
    out_spec = pl.BlockSpec((bm, bn), lambda m, n: (m, n))
    extra = [v for v in (part, res) if v is not None]
    return pl.pallas_call(
        functools.partial(project_back_kernel, len(acts), n_half, part is not None, res is not None),
        grid=(tokens // bm, dim // bn),
        in_specs=[pl.BlockSpec((n_half, bm, w), lambda m, n: (0, m, 0)) for w in widths]
        + [pl.BlockSpec((n_half, bn, w), lambda m, n: (0, n, 0)) for w in widths] + [out_spec] * len(extra),
        out_specs=out_spec,
        out_shape=jax.ShapeDtypeStruct((tokens, dim), BF16),
        compiler_params=pltpu.CompilerParams(dimension_semantics=("arbitrary", "arbitrary"), vmem_limit_bytes=VMEM_LIMIT),
        cost_estimate=cost(2 * tokens * dim * n_half * sum(widths), 2 * n_half * (tokens + 2 * dim) * sum(widths) + 4 * tokens * dim),
        name="project_back",
    )(*acts, *weights, *extra)


def input_grad_kernel(x_ref, dy_ref, dh_ref, gain_ref, dx_ref, dgain_ref):
    x_f = x_ref[...].astype(F32)
    d_h = dh_ref[...].astype(F32)
    inv_rms = lax.rsqrt(jnp.mean(x_f * x_f, axis=-1, keepdims=True) + NORM_EPS)
    grad_gain = d_h * gain_ref[...]
    mean_gx = jnp.mean(grad_gain * x_f, axis=-1, keepdims=True)
    dx_ref[...] = (dy_ref[...].astype(F32) + inv_rms * (grad_gain - x_f * inv_rms * inv_rms * mean_gx)).astype(BF16)

    @pl.when(pl.program_id(0) == 0)
    def _():
        dgain_ref[...] = jnp.zeros_like(dgain_ref)

    dgain_ref[...] += jnp.sum(d_h * x_f * inv_rms, axis=0, keepdims=True)


def input_grad(x, dy, d_h, gain):
    tokens, dim = x.shape
    block = 128
    row_spec = pl.BlockSpec((block, dim), lambda s: (s, 0))
    gain_spec = pl.BlockSpec((1, dim), lambda s: (0, 0))
    return pl.pallas_call(
        input_grad_kernel,
        grid=(tokens // block,),
        in_specs=[row_spec, row_spec, row_spec, gain_spec],
        out_specs=[row_spec, gain_spec],
        out_shape=[jax.ShapeDtypeStruct((tokens, dim), BF16), jax.ShapeDtypeStruct((1, dim), F32)],
        compiler_params=pltpu.CompilerParams(dimension_semantics=("arbitrary",), vmem_limit_bytes=VMEM_LIMIT),
        cost_estimate=cost(60 * tokens * dim, 8 * tokens * dim),
        name="input_grad",
    )(x, dy, d_h, gain.reshape(1, dim))


def flip_kernel(w_ref, *out_refs):
    width = w_ref.shape[0] // len(out_refs)
    for i, out_ref in enumerate(out_refs):
        out_ref[...] = w_ref[i * width:(i + 1) * width, :].T


def flip(w, parts):
    rows, cols = w.shape
    shape = jax.ShapeDtypeStruct((cols, rows // parts), BF16)
    return pl.pallas_call(flip_kernel, out_shape=[shape] * parts, cost_estimate=cost(10 * rows * cols, 4 * rows * cols), name="flip")(w)


def finish_kernel(n_parts, splits, *refs):
    parts, outs = refs[:n_parts], refs[n_parts:]
    for p, part in enumerate(parts):
        width = part.shape[1] // splits
        for i, out in enumerate(outs):
            out[:, p * width:(p + 1) * width] = part[:, i * width:(i + 1) * width].astype(BF16)


def finish(parts, splits):
    rows, width = parts[0].shape
    shape = jax.ShapeDtypeStruct((rows, len(parts) * width // splits), BF16)
    return pl.pallas_call(functools.partial(finish_kernel, len(parts), splits), out_shape=[shape] * splits, name="finish",
                          cost_estimate=cost(10 * rows * width, 6 * rows * width))(*parts)


def finish_flip_kernel(*refs):
    parts, out = refs[:-1], refs[-1]
    width = parts[0].shape[1]
    for p, part in enumerate(parts):
        out[p * width:(p + 1) * width, :] = part[...].T.astype(BF16)


def finish_flip(parts):
    rows, width = parts[0].shape
    shape = jax.ShapeDtypeStruct((len(parts) * width, rows), BF16)
    return pl.pallas_call(finish_flip_kernel, out_shape=shape, name="finish_flip",
                          cost_estimate=cost(10 * rows * width, 6 * rows * width))(*parts)


def after(dep, value):
    return lax.optimization_barrier((dep, value))[1]


def solution(mesh):
    tp = mesh.shape['tp']
    chips = mesh.shape['fsdp'] // CORES
    step_mesh = Mesh(mesh.devices.reshape(tp, chips, CORES), ('tp', 'chip', 'core'))
    across = ('tp', 'chip')
    fsdp = ('chip', 'core')
    act_spec = P(fsdp, 'tp', None)
    col_spec = P(fsdp, 'tp')
    row_spec = P('tp', fsdp)

    def shard_body(x_loc, gain, wq_loc, wk_loc, wv_loc, wo_loc, dy_loc):
        batch, seq, dim = x_loc.shape
        tokens = batch * seq
        q_cols, kv_cols = wq_loc.shape[1], wk_loc.shape[1]
        kw, qw = kv_cols // CORES, q_cols // CORES
        rows = wq_loc.shape[0]
        tp_idx, core = lax.axis_index('tp'), lax.axis_index('core')
        first = core == 0

        def swap(value):
            return lax.ppermute(value, 'core', [(0, 1), (1, 0)])

        def by_core(mine, other, axis):
            return jnp.concatenate([jnp.where(first, mine, other), jnp.where(first, other, mine)], axis=axis)

        def columns(block, width):
            return (lax.dynamic_slice_in_dim(block, core * width, width, axis=1),
                    lax.dynamic_slice_in_dim(block, (1 - core) * width, width, axis=1))

        def gather(mine, other):
            block = by_core(mine, swap(other), 0)
            return lax.all_gather(block, across, axis=0, tiled=True).reshape(tp, dim, block.shape[1])

        def scatter(parts):
            return lax.psum_scatter(parts.reshape(tp * dim, parts.shape[2]), across, scatter_dimension=0, tiled=True)

        def settle(grad):
            grad = grad.astype(BF16)
            mine = lax.dynamic_slice_in_dim(grad, core * rows, rows)
            other = swap(lax.dynamic_slice_in_dim(grad, (1 - core) * rows, rows))
            return jnp.where(first, mine, other), jnp.where(first, other, mine)

        x = x_loc.reshape(tokens, dim)
        dy = dy_loc.reshape(tokens, dim)
        k_mine, k_other = columns(wk_loc, kw)
        v_mine, v_other = columns(wv_loc, kw)
        wkv = gather(jnp.concatenate([k_mine, v_mine], axis=1), jnp.concatenate([k_other, v_other], axis=1))
        wq = gather(*columns(wq_loc, qw))
        flipped = flip(wo_loc, CORES)
        wo = gather(jnp.where(first, flipped[0], flipped[1]), jnp.where(first, flipped[1], flipped[0]))

        normed, normed_t, dy_t = prepare(x, dy, gain)
        acts = (normed, swap(normed))
        d_outs = (dy, swap(dy))
        acts_t = [normed_t, swap(normed_t)]
        d_outs_t = [dy_t, swap(dy_t)]

        cos_tab, sin_tab = rope_tables(seq * tp)
        tables = jnp.stack([lax.dynamic_slice_in_dim(cos_tab, tp_idx * seq, seq), lax.dynamic_slice_in_dim(sin_tab, tp_idx * seq, seq),
                            cos_tab[:seq], sin_tab[:seq]])
        second = tp_idx.astype(jnp.int32).reshape(1)

        def project(act, weights, dep):
            act = after(dep, act)
            return [dot_nn(act, weights[z]).astype(BF16) for z in range(tp)]

        def send_kv(kv):
            return [lax.ppermute(part, 'tp', [(0, 1)]) for part in kv]

        def attend_set(kv, kv_prev, q, d_mixed, dep):
            return attend(seq, second, after(dep, tables), q, kv, d_mixed, kv_prev)

        def kv_grad(own, prev):
            return (own + lax.ppermute(prev, 'tp', [(1, 0)]).astype(F32)).astype(BF16)

        kv0 = project(acts[0], wkv, normed)
        prev0 = send_kv(kv0)
        kv1 = project(acts[1], wkv, kv0[-1])
        prev1 = send_kv(kv1)
        q0 = project(acts[0], wq, kv1[-1])
        q1 = project(acts[1], wq, q0[-1])
        d_mixed0 = project(d_outs[0], wo, q1[-1])
        mixed0, d_q0, own0, back0 = attend_set(kv0, prev0, q0, d_mixed0, d_mixed0[-1])
        d_kv0 = kv_grad(own0, back0)
        d_mixed1 = project(d_outs[1], wo, mixed0)
        mixed1, d_q1, own1, back1 = attend_set(kv1, prev1, q1, d_mixed1, d_mixed1[-1])
        d_kv1 = kv_grad(own1, back1)

        part = weight_grad([after(mixed1, d_outs_t[0]), d_outs_t[1]], [mixed0, mixed1])
        dwo = scatter(part)
        part = weight_grad([after(part, acts_t[0]), acts_t[1]], [d_q0, d_q1])
        dwq = scatter(part)
        part = weight_grad([after(part, acts_t[0]), acts_t[1]], [d_kv0, d_kv1])
        dwkv = scatter(part)

        y_other = project_back([after(part, mixed1)], [wo])
        y_part = swap(y_other)
        dh_other = project_back([after(y_other, d_q1), d_kv1], [wq, wkv])
        dh_part = swap(dh_other)
        y = project_back([after(dh_other, mixed0)], [wo], part=y_part, res=x)
        d_normed = project_back([after(y, d_q0), d_kv0], [wq, wkv], part=dh_part)
        dx, d_gain = input_grad(x, dy, d_normed, gain)
        d_gain = lax.psum(d_gain.reshape(dim), ('tp', 'chip', 'core'))

        dwo_loc = finish_flip(settle(after(d_gain, dwo)))
        dwq_loc, = finish(settle(after(d_gain, dwq)), 1)
        dwk_loc, dwv_loc = finish(settle(after(d_gain, dwkv)), 2)
        return (y.reshape(x_loc.shape), dx.reshape(x_loc.shape), dwq_loc, dwk_loc, dwv_loc, dwo_loc, d_gain)

    return jax.shard_map(shard_body, mesh=step_mesh,
                         in_specs=(act_spec, P(), col_spec, col_spec, col_spec, row_spec, act_spec),
                         out_specs=(act_spec, act_spec, col_spec, col_spec, col_spec, row_spec, P()),
                         check_vma=False)
```
